32 devices in a mesh: row: 2 (over y), col: 4 (over z), depth: 4 (over x, core).
Axes of the slice: x: 2, y: 2, z: 4, core: 2. Of those that a mesh axis runs over, the one named last changes fastest.
Arguments:
- state_matrix: float32 [6144, 6144], P('row', 'col'), as said below
- gram_factor: float32 [6144, 256], P(('col', 'depth'), 'row'), as said below
Outputs:
- squared: float32 [6144, 6144], P('row', ('col', 'depth'))
- appended: float32 [6144, 256], P(('row', 'col', 'depth'))
- norm_ratio: float32 [256], replicated
Inputs may be any that keep to these rules, and one draw needn't show every extreme that they name: `gram_factor`: entries whose scale grows up to about ninefold along the rows; the columns differ in scale by up to tenfold. `state_matrix`: A real matrix with entries of order one on the diagonal and smaller ones elsewhere.
All inputs are finite; a program needn't handle non-finite values.
Results may differ from the reference program's by a relative error of at most 0.000073.
Values sent between devices are 32-bit elements; how exact they have to be, the bound alone decides.
No kernel may reach another device: no remote copies, remote signals or barrier semaphores. Data moves between devices by JAX's collectives and lax.ppermute only.
A program may use at most 128 MiB of HBM per device.

```python
import math
import jax
import jax.numpy as jnp
from jax import lax

ORDER = 6144
RANK = 256


def draw_state_matrix(key, part):
    first, second, third = jax.random.split(jax.random.fold_in(key, 11), 3)
    noise = jax.random.normal(first, (ORDER, ORDER), jnp.float32)
    magnitude = jax.random.uniform(second, (ORDER,), jnp.float32, 0.1, 0.9)
    signs = jnp.where(jax.random.uniform(third, (ORDER,), jnp.float32) < 0.5, -1.0, 1.0)
    return noise * (0.6 / math.sqrt(ORDER)) + jnp.diag(signs * magnitude)


def draw_gram_factor(key, part):
    first, second, third = jax.random.split(jax.random.fold_in(key, 23), 3)
    positions = jnp.arange(ORDER, dtype=jnp.float32) / ORDER
    row_scale = jnp.exp(math.log(3.0) * positions + jax.random.uniform(second, (ORDER,), jnp.float32, 0.0, math.log(3.0)))
    col_scale = jnp.exp(jax.random.uniform(third, (RANK,), jnp.float32, math.log(0.3), math.log(3.0)))
    noise = jax.random.normal(first, (ORDER, RANK), jnp.float32)
    return noise * row_scale[:, None] * col_scale[None, :]


def setup_inputs(seed: int = 0) -> dict:
    streams_of = jax.random.split(jax.random.key(seed), 3)
    state_matrix = draw_state_matrix(jax.random.fold_in(streams_of[2], 71), 0)
    gram_factor = draw_gram_factor(jax.random.fold_in(streams_of[2], 71), 0)
    return {"state_matrix": state_matrix, "gram_factor": gram_factor}


def reference(state_matrix, gram_factor):
    squared = jnp.dot(state_matrix, state_matrix, preferred_element_type=jnp.float32, precision=lax.Precision.HIGHEST)
    appended = jnp.dot(state_matrix, gram_factor, preferred_element_type=jnp.float32, precision=lax.Precision.HIGHEST)
    new_sq = lax.optimization_barrier(jnp.sum(appended * appended, axis=0))
    old_sq = lax.optimization_barrier(jnp.sum(gram_factor * gram_factor, axis=0))
    norm_ratio = jnp.sqrt(new_sq) / jnp.sqrt(old_sq + 1e-06)
    return (squared, appended, norm_ratio)
```

```python
import jax
import jax.numpy as jnp
from jax import lax
from jax.sharding import PartitionSpec as P


def product(left, right):
    return jnp.dot(left, right, preferred_element_type=jnp.float32, precision=lax.Precision.HIGH)


def halving_order(count):
    if count == 1:
        return [0]
    rest = halving_order(count // 2)
    return [2 * k for k in rest] + [2 * k + 1 for k in rest]


def to_partner(value, axis, step):
    count = lax.axis_size(axis)
    return lax.ppermute(value, axis, [(i, i ^ step) for i in range(count)])


def body(state_matrix, gram_factor):
    row_count = lax.axis_size("row")
    col_count = lax.axis_size("col")
    depth_count = lax.axis_size("depth")
    row_index = lax.axis_index("row")
    col_index = lax.axis_index("col")
    depth_index = lax.axis_index("depth")
    block_rows, block_cols = state_matrix.shape
    slab = block_cols // depth_count
    blocks_per_row = block_rows // block_cols
    chunk = block_rows // col_count
    order = halving_order(depth_count)
    half = depth_count // 2

    stacked = state_matrix.reshape(blocks_per_row, block_cols, block_cols)

    def own_rows(offsets):
        pieces = [
            lax.dynamic_slice(stacked, (0, depth_index * slab, (depth_index ^ k) * slab), (blocks_per_row, slab, slab))
            for k in offsets
        ]
        return jnp.concatenate(pieces, axis=2).reshape(blocks_per_row * slab, len(offsets) * slab)

    def over_rows(own):
        if row_count != 2:
            return lax.all_gather(own, "row", axis=0, tiled=True)
        other = to_partner(own, "row", 1)
        first = row_index == 0
        return jnp.concatenate([jnp.where(first, own, other), jnp.where(first, other, own)], axis=0)

    def finish(part, leaving):
        step = 2
        while step < depth_count:
            width = leaving.shape[1]
            part = part[:, :width] + to_partner(leaving, "depth", step)
            leaving = part[:, width // 2 :]
            step *= 2
        return part

    factor_block = lax.all_gather(gram_factor, "row", axis=1, tiled=True)
    factor_rows = lax.all_gather(factor_block, "col", axis=0, tiled=True)

    left = []
    for i in range(col_count):
        piece = lax.dynamic_slice(state_matrix, (i * chunk, depth_index * slab), (chunk, slab))
        if i == col_count - 1:
            piece, factor_rows = lax.optimization_barrier((piece, factor_rows))
        left.append(lax.all_gather(piece, "col", axis=1, tiled=True))

    right_send = over_rows(own_rows(order[half:]))
    right_keep = over_rows(own_rows(order[:half]))

    squared = []
    own_left = left[0]
    for i in range(col_count):
        block = left[i]
        if i > 0:
            block, leaving = lax.optimization_barrier((block, leaving))
            squared[-1] = finish(squared[-1], leaving)
            if i > 1:
                block, squared[-2] = lax.optimization_barrier((block, squared[-2]))
            own_left = jnp.where(col_index == i, block, own_left)
        received = to_partner(product(block, right_send), "depth", 1)
        part = product(block, right_keep) + received
        width = part.shape[1] // 2
        squared.append(part)
        leaving = part[:, width:]
    squared[-1] = finish(squared[-1], leaving)
    terms = product(own_left, factor_rows)

    size = chunk // depth_count
    pieces = [lax.dynamic_slice_in_dim(terms, (depth_index ^ k) * size, size, 0) for k in order]
    new_rows = jnp.concatenate(pieces, axis=0)
    step = 1
    while step < depth_count:
        size = new_rows.shape[0] // 2
        new_rows = new_rows[:size] + to_partner(new_rows[size:], "depth", step)
        step *= 2

    new_sq = jnp.sum(new_rows * new_rows, axis=0)
    old_sq = jnp.sum(factor_block * factor_block, axis=0) * (1.0 / row_count)
    totals_new, totals_old = lax.psum((new_sq, old_sq), ("row", "col", "depth"))
    norm_ratio = jnp.sqrt(totals_new) / jnp.sqrt(totals_old + 1e-06)
    return (jnp.concatenate(squared, axis=0), new_rows, norm_ratio)


def solution(mesh):
    in_specs = (P("row", "col"), P(("col", "depth"), "row"))
    out_specs = (P("row", ("col", "depth")), P(("row", "col", "depth"), None), P())
    return jax.shard_map(body, mesh=mesh, in_specs=in_specs, out_specs=out_specs, check_vma=False)
```
